32 devices in a mesh: mem: 8 (over y, x, core), tile: 4 (over z).
Axes of the slice: x: 2, y: 2, z: 4, core: 2. Of those that a mesh axis runs over, the one named last changes fastest.
Arguments:
- perturbations: bfloat16 [16, 4, 128, 1024], P('mem', None, 'tile'), may hold values from -6 to 6
- right_side: float32 [4, 128, 1024], P(None, 'tile'), may hold values from -14 to 14
- fine_taps: float32 [2, 4, 5], replicated, may hold values from 0.3 to 1
- coarse_lat: float32 [32, 32], replicated, may hold values from -4 to 16, as said below
- coarse_lon: float32 [256, 256], replicated, may hold values from -4 to 16, as said below
Outputs:
- solution: float32 [4, 128, 1024], P(None, 'tile', 'mem')
- residual: float32 [4, 128, 1024], P(None, 'tile', 'mem')
The draws below stay inside these ranges and needn't reach their ends.
Inputs may be any that keep to these rules, and one draw needn't show every extreme that they name: `coarse_lat`: symmetric. `coarse_lon`: symmetric.
All inputs are finite; a program needn't handle non-finite values.
Results may differ from the reference program's by a relative error of at most 0.0003.
Values may be sent and summed in bfloat16 or wider, within the bound.
A program may use at most 64 MiB of HBM per device.

```python
import jax
import jax.numpy as jnp
from jax import lax

LON = 1024
LEV = 4
ITERS = 2
MEMBERS = 16
LAT = 128
CLAT = 32
CLON = 256


def coarse_matrix(key, order_size, decay_len):
    positions = jnp.arange(order_size)
    distance = jnp.abs(positions[:, None] - positions[None, :]).astype(jnp.float32)
    uniform_draw = jax.random.uniform(key, (order_size, order_size), jnp.float32, -1.0, 1.0)
    off_diag = 0.5 * (uniform_draw + uniform_draw.T) * jnp.exp(-distance / decay_len) * (1.0 - jnp.eye(order_size, dtype=jnp.float32))
    row_weight = 1.0 + jnp.sum(jnp.abs(off_diag), axis=1)
    return 4.0 * (off_diag + jnp.diag(row_weight)) / jnp.mean(row_weight)


def draw_coarse_lat(key, part):
    return coarse_matrix(jax.random.fold_in(key, 17), CLAT, CLAT / 4.0)


def draw_coarse_lon(key, part):
    return coarse_matrix(jax.random.fold_in(key, 29), CLON, CLON / 4.0)


def draw_right_side(key, part):
    lat_pos = jnp.arange(LAT, dtype=jnp.float32)[None, :, None] / LAT
    lon_pos = jnp.arange(LON, dtype=jnp.float32)[None, None, :] / LON
    noise_draw = jnp.clip(jax.random.normal(jax.random.fold_in(key, 7), (LEV, LAT, LON), jnp.float32), -4.0, 4.0)
    return noise_draw * jnp.exp(0.6 * lat_pos + 0.6 * lon_pos)


def strengthened(values, key, source, target, parts, factor):
    owner, partner = [(jnp.arange(values.shape[position]) // (values.shape[position] // parts)).reshape([-1 if axis == position else 1 for axis in range(values.ndim)]) for position in (source, target)]
    chosen = jax.random.permutation(key, parts)[partner]
    strong = (owner == chosen) | (owner == (partner + parts // 2) % parts)
    return jnp.where(strong, factor * values, values)


def shard_levels(key, dims, cuts, smallest, high):
    gain = 1.0
    for position, blocks in cuts:
        heights = jax.random.uniform(jax.random.fold_in(jax.random.fold_in(key, 6), position), (blocks,), jnp.float32, smallest / len(cuts), high / len(cuts))
        gain = gain * jnp.repeat(jnp.exp(heights), dims[position] // blocks).reshape((-1,) + (1,) * (len(dims) - 1 - position))
    return gain


def heavy_noise(own_key, shape, scale, most, cuts, heavy, kind=jnp.bfloat16):
    values = scale * jax.random.normal(own_key, shape, jnp.float32)
    if cuts:
        values = values * shard_levels(own_key, shape, cuts, -0.22, 0.18)
    return jnp.clip(strengthened(values, jax.random.fold_in(own_key, 3), *heavy), -most, most).astype(kind)


def setup_inputs(seed: int = 0) -> dict:
    splits = jax.random.split(jax.random.key(seed), 6)
    perturbations = heavy_noise(splits[0], (MEMBERS, LEV, LAT, LON), 1.0, 6.0, ((0, 8), (2, 4)), (0, 3, 8, 2.0))
    right_side = draw_right_side(jax.random.fold_in(splits[5], 71), 0)
    fine_taps = jnp.clip(jax.random.uniform(splits[2], (2, LEV, 5), jnp.float32, 0.3, 1.0), 0.3, 1.0)
    coarse_lat = draw_coarse_lat(jax.random.fold_in(splits[5], 71), 0)
    coarse_lon = draw_coarse_lon(jax.random.fold_in(splits[5], 71), 0)
    return {"perturbations": perturbations, "right_side": right_side, "fine_taps": fine_taps, "coarse_lat": coarse_lat, "coarse_lon": coarse_lon}


exact_mode = lax.Precision.HIGHEST

def normalized(fine_taps):
    energy = fine_taps[:, :, 0] ** 2 + 2.0 * lax.optimization_barrier(jnp.sum(fine_taps[:, :, 1:] ** 2, axis=2))
    return fine_taps / jnp.sqrt(energy)[:, :, None]

def lat_pass(values, kernel):
    height = values.shape[1]
    padded = jnp.pad(values, ((0, 0), (4, 4), (0, 0)))
    result = kernel[:, 0, None, None] * values
    for offset in range(1, 5):
        result = result + kernel[:, offset, None, None] * (padded[:, 4 + offset:4 + offset + height] + padded[:, 4 - offset:4 - offset + height])
    return result

def lon_pass(values, kernel):
    result = kernel[:, 0, None, None] * values
    for offset in range(1, 5):
        result = result + kernel[:, offset, None, None] * (jnp.roll(values, offset, axis=2) + jnp.roll(values, -offset, axis=2))
    return result

def block_mean(values):
    levels, height, extent = values.shape
    return lax.optimization_barrier(jnp.mean(values.reshape(levels, height // 4, 4, extent // 4, 4), axis=(2, 4)))

def prolong(coarse):
    levels, height, extent = coarse.shape
    return jnp.broadcast_to(coarse[:, :, None, :, None], (levels, height, 4, extent, 4)).reshape(levels, height * 4, extent * 4)

def smooth(coarse, coarse_lat, coarse_lon):
    across = jnp.einsum('ab,lbc->lac', coarse_lat, coarse, precision=exact_mode)
    return jnp.einsum('lac,cd->lad', across, coarse_lon, precision=exact_mode)

def reference(perturbations, right_side, fine_taps, coarse_lat, coarse_lon):
    kernel = normalized(fine_taps)
    members = perturbations.shape[0]

    def apply_operator(vector):

        def advance(summed, member):
            spread = member.astype(jnp.float32)
            weighted = spread * vector
            coarse = block_mean(weighted)
            detail = weighted - prolong(coarse)
            detail = lat_pass(lat_pass(detail, kernel[0]), kernel[0])
            detail = lon_pass(lon_pass(detail, kernel[1]), kernel[1])
            blended = detail - prolong(block_mean(detail)) + prolong(smooth(coarse, coarse_lat, coarse_lon))
            return (summed + spread * blended, None)
        summed, _ = lax.scan(advance, jnp.zeros_like(vector), perturbations)
        return vector + summed / (members - 1)
    solution = jnp.zeros_like(right_side)
    residual = right_side
    squares = jnp.sum(residual * residual)
    for iteration in range(ITERS):
        applied = apply_operator(residual)
        step_size = squares / jnp.sum(residual * applied)
        solution = solution + step_size * residual
        residual = residual - step_size * applied
        squares = jnp.sum(residual * residual)
    return (solution, residual)
```

```python
import functools

import jax
import jax.numpy as jnp
from jax import lax
from jax.experimental import pallas as pl
from jax.experimental.pallas import tpu as pltpu
from jax.sharding import PartitionSpec as P

ITERS = 2
HALO = 8
LANES = 128
MESH = pl.DeviceIdType.MESH

exact_mode = lax.Precision.HIGHEST


def kernel_body(
    sizes,
    x_in,
    r_in,
    taps_in,
    lat_in,
    lon_in,
    sol_out,
    res_out,
    xe,
    re,
    rmsg,
    rhalo,
    det,
    mid,
    fine,
    coarse,
    smooth,
    part,
    rs_recv,
    rshare,
    asend,
    arecv,
    scal,
    sem_x,
    sem_r,
    sem_c,
    sem_rs,
    sem_ag,
    sem_h,
    sem_s,
):
    groups, tiles, levels, height, extent, members = sizes
    me = lax.axis_index("mem")
    tile = lax.axis_index("tile")
    fields = 8
    half = height // 2
    phase = extent // 4
    quarter = extent // groups // 4
    crows = height // 4
    hq = HALO // 2
    devices = groups * tiles
    flat = me * tiles + tile
    not_first = tile > 0
    not_last = tile < tiles - 1

    sub = lax.broadcasted_iota(jnp.int32, (fields, LANES), 0)
    lane = lax.broadcasted_iota(jnp.int32, (fields, LANES), 1)
    low = sub < levels
    low_p = lax.broadcasted_iota(jnp.int32, (fields, phase), 0) < levels
    level_of = lax.rem(lax.broadcasted_iota(jnp.int32, (fields, phase), 0), levels)

    def copy(src, dst, sems, slot_send, slot_recv, target):
        return pltpu.make_async_remote_copy(
            src_ref=src,
            dst_ref=dst,
            send_sem=sems.at[slot_send],
            recv_sem=sems.at[slot_recv],
            device_id=target,
            device_id_type=MESH,
        )

    def swap(v):
        return pltpu.roll(v, levels, 0)

    barrier = pltpu.get_barrier_semaphore()

    def greet(k, carry):
        other = lax.rem(flat + k, devices)
        pl.semaphore_signal(
            barrier,
            inc=1,
            device_id=(other // tiles, lax.rem(other, tiles)),
            device_id_type=MESH,
        )
        return carry

    lax.fori_loop(1, devices, greet, 0)

    kern = []
    for d in range(2):
        raw = []
        for o in range(5):
            v = jnp.full((fields, phase), taps_in[d, 0, o], jnp.float32)
            for l in range(1, levels):
                v = jnp.where(level_of == l, taps_in[d, l, o], v)
            raw.append(v)
        energy = raw[0] * raw[0] + 2.0 * (
            raw[1] * raw[1] + raw[2] * raw[2] + raw[3] * raw[3] + raw[4] * raw[4]
        )
        root = jnp.sqrt(energy)
        kern.append([v / root for v in raw])

    def pack_rows(k, carry):
        a = r_in[half - HALO + k]
        b = r_in[half - hq + k]
        lowx = lax.broadcasted_iota(jnp.int32, (fields, extent), 0) < levels
        rmsg[0, k] = jnp.where(lowx, swap(a), b)
        rmsg[1, k] = jnp.where(lowx, r_in[k], swap(r_in[hq + k]))
        return carry

    lax.fori_loop(0, hq, pack_rows, 0)
    xe[pl.ds(HALO, height)] = x_in[...]

    zero_x = jnp.zeros((HALO, fields, extent), xe.dtype)
    zero_r = jnp.zeros((hq, fields, extent), jnp.float32)

    @pl.when(jnp.logical_not(not_first))
    def _():
        xe[pl.ds(0, HALO)] = zero_x
        rhalo[0] = zero_r
        for g in range(groups):
            arecv[g, pl.ds(half, hq)] = jnp.zeros((hq, fields, LANES), jnp.float32)

    @pl.when(jnp.logical_not(not_last))
    def _():
        xe[pl.ds(HALO + height, HALO)] = zero_x
        rhalo[1] = zero_r
        for g in range(groups):
            arecv[g, pl.ds(half + hq, hq)] = jnp.zeros((hq, fields, LANES), jnp.float32)

    pl.semaphore_wait(barrier, devices - 1)

    x_down = copy(
        x_in.at[pl.ds(height - HALO, HALO)], xe.at[pl.ds(0, HALO)], sem_x, 0, 1, (me, tile + 1)
    )
    x_up = copy(
        x_in.at[pl.ds(0, HALO)], xe.at[pl.ds(HALO + height, HALO)], sem_x, 2, 3, (me, tile - 1)
    )
    r_down = copy(rmsg.at[0], rhalo.at[0], sem_r, 0, 1, (me, tile + 1))
    r_up = copy(rmsg.at[1], rhalo.at[1], sem_r, 2, 3, (me, tile - 1))

    @pl.when(not_last)
    def _():
        x_down.start()
        r_down.start()

    @pl.when(not_first)
    def _():
        x_up.start()
        r_up.start()

    def spread(source, base_low, base_high, count):
        def row(k, carry):
            v = source[k]
            w = swap(v)
            lowx = lax.broadcasted_iota(jnp.int32, (fields, extent), 0) < levels
            re[base_low + k] = jnp.where(lowx, v, w)
            re[base_high + k] = jnp.where(lowx, w, v)
            return carry

        lax.fori_loop(0, count, row, 0)

    def slices(rows):
        outs = []
        for g in range(groups):
            chunk, off = (quarter * g) // LANES, (quarter * g) % LANES
            value = None
            for p in range(4):
                piece = rows[p][:, chunk * LANES : (chunk + 1) * LANES]
                shift = (p * quarter - off) % LANES
                if shift:
                    piece = pltpu.roll(piece, shift, 1)
                value = piece if value is None else jnp.where(lane >= p * quarter, piece, value)
            outs.append(value)
        return outs

    spread(r_in, HALO, HALO + half, half)

    def own_share(k, carry):
        outs = slices([r_in[k, :, p * phase : (p + 1) * phase] for p in range(4)])
        for g in range(groups):
            rshare[g, k] = outs[g]
        return carry

    lax.fori_loop(0, half, own_share, 0)
    res_out[...] = rshare[me]

    def detail_block(it, block, own):
        base = 4 * block
        for_sum = None
        weighted = []
        for p in range(4):
            cols = slice(p * phase, (p + 1) * phase)
            ws = [
                xe[base + j, :, cols].astype(jnp.float32) * re[base + j, :, cols] for j in range(4)
            ]
            weighted.append(ws)
            s = (ws[0] + ws[1]) + (ws[2] + ws[3])
            for_sum = s if for_sum is None else for_sum + s
        mean = for_sum * 0.0625
        if own:
            coarse[it, tile, block - HALO // 4] = mean
        for p in range(4):
            for j in range(4):
                det[base + j, :, p * phase : (p + 1) * phase] = weighted[p][j] - mean

    def lat_block(src, dst, block, factor):
        base = 4 * block
        for p in range(4):
            cols = slice(p * phase, (p + 1) * phase)
            rows = [src[base + j, :, cols] for j in range(12)]
            for j in range(4):
                v = kern[0][0] * rows[j + 4]
                for o in range(1, 5):
                    v = v + kern[0][o] * (rows[j + 4 + o] + rows[j + 4 - o])
                if factor is not None:
                    v = v * factor
                dst[base + j, :, cols] = v

    def lon_pass(v):
        plus = [pltpu.roll(a, phase - 1, 1) for a in v]
        minus = [pltpu.roll(a, 1, 1) for a in v]
        table = {0: v, 1: plus, -1: minus}

        def at(t):
            return table[t // 4][t % 4]

        outs = []
        for p in range(4):
            u = kern[1][0] * v[p]
            for o in range(1, 5):
                u = u + kern[1][o] * (at(p + o) + at(p - o))
            outs.append(u)
        return outs

    def lon_row(i, carry):
        v = [fine[i, :, p * phase : (p + 1) * phase] for p in range(4)]
        v = lon_pass(lon_pass(v))
        for p in range(4):
            fine[i, :, p * phase : (p + 1) * phase] = v[p]
        return carry

    for it in range(ITERS):
        def own_block(b, carry):
            detail_block(it, b, True)
            return carry

        lax.fori_loop(HALO // 4, HALO // 4 + crows, own_block, 0)

        def coarse_send(k, carry):
            other = lax.rem(tile + k, tiles)
            copy(
                coarse.at[it, tile],
                coarse.at[it, tile],
                sem_c.at[it],
                (0, other),
                (1, tile),
                (me, other),
            ).start()
            return carry

        lax.fori_loop(1, tiles, coarse_send, 0)

        if it == 0:

            @pl.when(not_first)
            def _():
                x_down.wait_recv()
                r_down.wait_recv()

            @pl.when(not_last)
            def _():
                x_up.wait_recv()
                r_up.wait_recv()

            spread(rhalo.at[0], 0, hq, hq)
            spread(rhalo.at[1], HALO + height, HALO + height + hq, hq)
        for b in range(HALO // 4):
            detail_block(it, b, False)
            detail_block(it, HALO // 4 + crows + b, False)

        last_block = crows + 1

        def lat_first(b, carry):
            outside = jnp.logical_or(
                jnp.logical_and(b == 0, tile == 0),
                jnp.logical_and(b == last_block, tile == tiles - 1),
            )
            lat_block(det, mid, b, jnp.where(outside, 0.0, 1.0).astype(jnp.float32))
            return carry

        lax.fori_loop(0, crows + 2, lat_first, 0)

        def lat_second(b, carry):
            lat_block(mid, fine, b, None)
            return carry

        lax.fori_loop(0, crows, lat_second, 0)
        lax.fori_loop(0, height, lon_row, 0)

        def coarse_wait(k, carry):
            other = lax.rem(tile + k, tiles)
            copy(
                coarse.at[it, other],
                coarse.at[it, other],
                sem_c.at[it],
                (0, other),
                (1, other),
                (me, other),
            ).wait()
            return carry

        lax.fori_loop(1, tiles, coarse_wait, 0)

        def across_tile(t, total):
            total = list(total)
            for b in range(crows):
                v = coarse[it, t, b]
                for a in range(crows):
                    total[a] = total[a] + lat_in[tile * crows + a, t * crows + b] * v
            return tuple(total)

        zero_c = jnp.zeros((fields, phase), jnp.float32)
        across = lax.fori_loop(0, tiles, across_tile, (zero_c,) * crows)
        smooth[...] = jnp.dot(
            jnp.concatenate(across, axis=0),
            lon_in[...],
            precision=exact_mode,
            preferred_element_type=jnp.float32,
        ).reshape(crows, fields, phase)

        def member_sum(block):
            base = 4 * block
            mean = None
            for p in range(4):
                fs = [fine[base + j, :, p * phase : (p + 1) * phase] for j in range(4)]
                s = (fs[0] + fs[1]) + (fs[2] + fs[3])
                mean = s if mean is None else mean + s
            extra = smooth[block] - mean * 0.0625
            rows = []
            for j in range(4):
                row = []
                for p in range(4):
                    cols = slice(p * phase, (p + 1) * phase)
                    u = xe[HALO + base + j, :, cols].astype(jnp.float32) * (
                        fine[base + j, :, cols] + extra
                    )
                    row.append(u + swap(u))
                rows.append(row)
            return rows

        def combine(b, carry):
            first = member_sum(b)
            second = member_sum(b + crows // 2)
            for j in range(4):
                packed = [jnp.where(low_p, first[j][p], second[j][p]) for p in range(4)]
                outs = slices(packed)
                for g in range(groups):
                    part[it, g, 4 * b + j] = outs[g]
            return carry

        lax.fori_loop(0, crows // 2, combine, 0)

        def rs_copy(other, source):
            return copy(
                part.at[it, other],
                rs_recv.at[it, source],
                sem_rs.at[it],
                (0, other),
                (1, source),
                (other, tile),
            )

        def rs_send(k, carry):
            rs_copy(lax.rem(me + k, groups), me).start()
            return carry

        lax.fori_loop(1, groups, rs_send, 0)
        total = part[it, me]

        def rs_wait(k, total):
            other = lax.rem(me + k, groups)
            rs_copy(other, other).wait()
            return total + rs_recv[it, other]

        total = lax.fori_loop(1, groups, rs_wait, total)
        applied = res_out[...] + total / (members - 1)
        residual = res_out[...]
        squares = jnp.sum(residual * residual, axis=0)
        inner = jnp.sum(residual * applied, axis=0)
        scal[it, flat] = jnp.where(low, squares + swap(squares), inner + swap(inner))

        def scal_copy(other, source):
            return copy(
                scal.at[it, flat],
                scal.at[it, source],
                sem_s.at[it],
                (0, other),
                (1, source),
                (other // tiles, lax.rem(other, tiles)),
            )

        def scal_send(k, carry):
            scal_copy(lax.rem(flat + k, devices), flat).start()
            return carry

        lax.fori_loop(1, devices, scal_send, 0)

        last = it + 1 == ITERS
        asend[pl.ds(0, half)] = applied
        if not last:
            arecv[me, pl.ds(0, half)] = applied
            for k in range(hq):
                asend[half + k] = jnp.where(
                    low, swap(asend[half - HALO + k]), asend[half - hq + k]
                )
                asend[half + hq + k] = jnp.where(low, asend[k], swap(asend[hq + k]))

            def ag_copy(other, source):
                return copy(
                    asend.at[pl.ds(0, half)],
                    arecv.at[source, pl.ds(0, half)],
                    sem_ag,
                    (0, other),
                    (1, source),
                    (other, tile),
                )

            def down_copy(other, source):
                return copy(
                    asend.at[pl.ds(half, hq)],
                    arecv.at[source, pl.ds(half, hq)],
                    sem_h.at[0],
                    (0, other),
                    (1, source),
                    (other, tile + 1),
                )

            def up_copy(other, source):
                return copy(
                    asend.at[pl.ds(half + hq, hq)],
                    arecv.at[source, pl.ds(half + hq, hq)],
                    sem_h.at[1],
                    (0, other),
                    (1, source),
                    (other, tile - 1),
                )

            def over_groups(condition, start, action):
                @pl.when(condition)
                def _():
                    def step(k, carry):
                        action(lax.rem(me + k, groups))
                        return carry

                    lax.fori_loop(start, groups, step, 0)

            always = tile >= 0
            over_groups(not_last, 0, lambda g: down_copy(g, me).start())
            over_groups(not_first, 0, lambda g: up_copy(g, me).start())
            over_groups(always, 1, lambda g: ag_copy(g, me).start())

        def scal_wait(k, carry):
            other = lax.rem(flat + k, devices)
            scal_copy(other, other).wait()
            return carry

        lax.fori_loop(1, devices, scal_wait, 0)
        sums = lax.fori_loop(
            0, devices, lambda d, t: t + scal[it, d], jnp.zeros((fields, LANES), jnp.float32)
        )
        zero = jnp.zeros_like(sums)
        squares = jnp.sum(jnp.where(low, sums, zero), axis=(0, 1), keepdims=True)
        inner = jnp.sum(jnp.where(low, zero, sums), axis=(0, 1), keepdims=True)
        step_size = jnp.broadcast_to(squares / inner, (fields, LANES))
        moved = step_size[None] * residual
        sol_out[...] = moved if it == 0 else sol_out[...] + moved
        res_out[...] = residual - step_size[None] * asend[pl.ds(0, half)]

        if not last:
            over_groups(not_first, 0, lambda g: down_copy(g, g).wait_recv())
            over_groups(not_last, 0, lambda g: up_copy(g, g).wait_recv())
            over_groups(always, 1, lambda g: ag_copy(g, g).wait_recv())
            per = LANES // quarter

            def update(k_base, count, base_low, base_high):
                def row(k, carry):
                    for c in range(phase // LANES):
                        got = [arecv[c * per + i, k_base + k] for i in range(per)]
                        for p in range(4):
                            value = None
                            for i in range(per):
                                shift = ((i - p) * quarter) % LANES
                                piece = pltpu.roll(got[i], shift, 1) if shift else got[i]
                                value = (
                                    piece
                                    if value is None
                                    else jnp.where(lane >= i * quarter, piece, value)
                                )
                            value = step_size * value
                            other = swap(value)
                            at = p * phase + c * LANES
                            cols = slice(at, at + LANES)
                            re[base_low + k, :, cols] = re[base_low + k, :, cols] - jnp.where(
                                low, value, other
                            )
                            re[base_high + k, :, cols] = re[base_high + k, :, cols] - jnp.where(
                                low, other, value
                            )
                    return carry

                lax.fori_loop(0, count, row, 0)

            update(0, half, HALO, HALO + half)
            update(half, hq, 0, hq)
            update(half + hq, hq, HALO + height, HALO + height + hq)
            over_groups(not_last, 0, lambda g: down_copy(g, g).wait_send())
            over_groups(not_first, 0, lambda g: up_copy(g, g).wait_send())
            over_groups(always, 1, lambda g: ag_copy(g, g).wait_send())

    @pl.when(not_last)
    def _():
        x_down.wait_send()
        r_down.wait_send()

    @pl.when(not_first)
    def _():
        x_up.wait_send()
        r_up.wait_send()


def local(perturbations, right_side, fine_taps, coarse_lat, coarse_lon):
    count_local, levels, height, extent = perturbations.shape
    groups, tiles = lax.axis_size("mem"), lax.axis_size("tile")
    members = count_local * groups
    fields = count_local * levels
    half, phase, share = height // 2, extent // 4, extent // groups
    hq, crows, devices = HALO // 2, height // 4, groups * tiles
    assert fields == 8 and share <= LANES and LANES % (share // 4) == 0 and half >= HALO

    natural = jnp.arange(extent)
    order = (natural % 4) * phase + natural // 4
    gather = order[:, None] == natural[None, :]
    x = jnp.einsum(
        "blin,nm->iblm",
        perturbations,
        gather.astype(jnp.bfloat16),
        preferred_element_type=jnp.bfloat16,
    ).reshape(height, fields, extent)
    r = jnp.einsum(
        "lhin,nm->ihlm",
        right_side.reshape(levels, 2, half, extent),
        gather.astype(jnp.float32),
        precision=exact_mode,
    ).reshape(half, fields, extent)

    f32 = jnp.float32
    vmem = pl.BlockSpec(memory_space=pltpu.VMEM)
    smem = pl.BlockSpec(memory_space=pltpu.SMEM)
    sizes = (groups, tiles, levels, height, extent, members)
    dma = pltpu.SemaphoreType.DMA
    sol, res = pl.pallas_call(
        functools.partial(kernel_body, sizes),
        out_shape=[jax.ShapeDtypeStruct((half, fields, LANES), f32)] * 2,
        in_specs=[vmem, vmem, smem, smem, vmem],
        out_specs=[vmem, vmem],
        scratch_shapes=[
            pltpu.VMEM((height + 2 * HALO, fields, extent), jnp.bfloat16),
            pltpu.VMEM((height + 2 * HALO, fields, extent), f32),
            pltpu.VMEM((2, hq, fields, extent), f32),
            pltpu.VMEM((2, hq, fields, extent), f32),
            pltpu.VMEM((height + 2 * HALO, fields, extent), f32),
            pltpu.VMEM((height + HALO, fields, extent), f32),
            pltpu.VMEM((height, fields, extent), f32),
            pltpu.VMEM((ITERS, tiles, crows, fields, phase), f32),
            pltpu.VMEM((crows, fields, phase), f32),
            pltpu.VMEM((ITERS, groups, half, fields, LANES), f32),
            pltpu.VMEM((ITERS, groups, half, fields, LANES), f32),
            pltpu.VMEM((groups, half, fields, LANES), f32),
            pltpu.VMEM((half + 2 * hq, fields, LANES), f32),
            pltpu.VMEM((groups, half + 2 * hq, fields, LANES), f32),
            pltpu.VMEM((ITERS, devices, fields, LANES), f32),
            dma((4,)),
            dma((4,)),
            dma((ITERS, 2, tiles)),
            dma((ITERS, 2, groups)),
            dma((2, groups)),
            dma((2, 2, groups)),
            dma((ITERS, 2, devices)),
        ],
        compiler_params=pltpu.CompilerParams(
            collective_id=0, has_side_effects=True, vmem_limit_bytes=60000 * 1024
        ),
        name="descent",
    )(x, r, fine_taps, coarse_lat, coarse_lon)

    spot = jnp.arange(share)
    place = (spot[:, None] % (share // 4)) * 4 + spot[:, None] // (share // 4) == spot[None, :]

    def natural_order(v):
        v = v[:, :, :share].reshape(half, 2, levels, share)
        return jnp.einsum(
            "ihlm,mn->lhin", v, place.astype(jnp.float32), precision=exact_mode
        ).reshape(levels, height, share)

    return natural_order(sol), natural_order(res)


def solution(mesh):
    placed = (P("mem", None, "tile", None), P(None, "tile", None), P(), P(), P())
    return jax.shard_map(
        local,
        mesh=mesh,
        in_specs=placed,
        out_specs=(P(None, "tile", "mem"), P(None, "tile", "mem")),
        check_vma=False,
    )
```

```python
import functools

import jax
import jax.numpy as jnp
from jax import lax
from jax.experimental import pallas as pl
from jax.experimental.pallas import tpu as pltpu
from jax.sharding import PartitionSpec as P

ITERS = 2
HALO = 8
LANES = 128
MESH = pl.DeviceIdType.MESH

exact_mode = lax.Precision.HIGHEST


def kernel_body(
    sizes,
    x_in,
    r_in,
    taps_in,
    lat_in,
    lon_in,
    sol_out,
    res_out,
    xe,
    re,
    rmsg,
    rhalo,
    det,
    mid,
    fine,
    coarse,
    smooth,
    part,
    rs_recv,
    rshare,
    asend,
    arecv,
    scal,
    sem_x,
    sem_r,
    sem_c,
    sem_rs,
    sem_ag,
    sem_h,
    sem_s,
):
    groups, tiles, levels, height, extent, members = sizes
    me = lax.axis_index("mem")
    tile = lax.axis_index("tile")
    fields = 8
    half = height // 2
    phase = extent // 4
    quarter = extent // groups // 4
    crows = height // 4
    hq = HALO // 2
    devices = groups * tiles
    flat = me * tiles + tile
    not_first = tile > 0
    not_last = tile < tiles - 1

    sub = lax.broadcasted_iota(jnp.int32, (fields, LANES), 0)
    lane = lax.broadcasted_iota(jnp.int32, (fields, LANES), 1)
    low = sub < levels
    low_p = lax.broadcasted_iota(jnp.int32, (fields, phase), 0) < levels
    level_of = lax.rem(lax.broadcasted_iota(jnp.int32, (fields, phase), 0), levels)

    def copy(src, dst, sems, slot_send, slot_recv, target):
        return pltpu.make_async_remote_copy(
            src_ref=src,
            dst_ref=dst,
            send_sem=sems.at[slot_send],
            recv_sem=sems.at[slot_recv],
            device_id=target,
            device_id_type=MESH,
        )

    def swap(v):
        return pltpu.roll(v, levels, 0)

    barrier = pltpu.get_barrier_semaphore()

    def greet(k, carry):
        other = lax.rem(flat + k, devices)
        pl.semaphore_signal(
            barrier,
            inc=1,
            device_id=(other // tiles, lax.rem(other, tiles)),
            device_id_type=MESH,
        )
        return carry

    lax.fori_loop(1, devices, greet, 0)

    kern = []
    for d in range(2):
        raw = []
        for o in range(5):
            v = jnp.full((fields, phase), taps_in[d, 0, o], jnp.float32)
            for l in range(1, levels):
                v = jnp.where(level_of == l, taps_in[d, l, o], v)
            raw.append(v)
        energy = raw[0] * raw[0] + 2.0 * (
            raw[1] * raw[1] + raw[2] * raw[2] + raw[3] * raw[3] + raw[4] * raw[4]
        )
        root = jnp.sqrt(energy)
        kern.append([v / root for v in raw])

    def pack_rows(k, carry):
        a = r_in[half - HALO + k]
        b = r_in[half - hq + k]
        lowx = lax.broadcasted_iota(jnp.int32, (fields, extent), 0) < levels
        rmsg[0, k] = jnp.where(lowx, swap(a), b)
        rmsg[1, k] = jnp.where(lowx, r_in[k], swap(r_in[hq + k]))
        return carry

    lax.fori_loop(0, hq, pack_rows, 0)
    xe[pl.ds(HALO, height)] = x_in[...]

    zero_x = jnp.zeros((HALO, fields, extent), xe.dtype)
    zero_r = jnp.zeros((hq, fields, extent), jnp.float32)

    @pl.when(jnp.logical_not(not_first))
    def _():
        xe[pl.ds(0, HALO)] = zero_x
        rhalo[0] = zero_r
        for g in range(groups):
            arecv[g, pl.ds(half, hq)] = jnp.zeros((hq, fields, LANES), jnp.float32)

    @pl.when(jnp.logical_not(not_last))
    def _():
        xe[pl.ds(HALO + height, HALO)] = zero_x
        rhalo[1] = zero_r
        for g in range(groups):
            arecv[g, pl.ds(half + hq, hq)] = jnp.zeros((hq, fields, LANES), jnp.float32)

    pl.semaphore_wait(barrier, devices - 1)

    x_down = copy(
        x_in.at[pl.ds(height - HALO, HALO)], xe.at[pl.ds(0, HALO)], sem_x, 0, 1, (me, tile + 1)
    )
    x_up = copy(
        x_in.at[pl.ds(0, HALO)], xe.at[pl.ds(HALO + height, HALO)], sem_x, 2, 3, (me, tile - 1)
    )
    r_down = copy(rmsg.at[0], rhalo.at[0], sem_r, 0, 1, (me, tile + 1))
    r_up = copy(rmsg.at[1], rhalo.at[1], sem_r, 2, 3, (me, tile - 1))

    @pl.when(not_last)
    def _():
        x_down.start()
        r_down.start()

    @pl.when(not_first)
    def _():
        x_up.start()
        r_up.start()

    def spread(source, base_low, base_high, count):
        def row(k, carry):
            v = source[k]
            w = swap(v)
            lowx = lax.broadcasted_iota(jnp.int32, (fields, extent), 0) < levels
            re[base_low + k] = jnp.where(lowx, v, w)
            re[base_high + k] = jnp.where(lowx, w, v)
            return carry

        lax.fori_loop(0, count, row, 0)

    def slices(rows):
        outs = []
        for g in range(groups):
            chunk, off = (quarter * g) // LANES, (quarter * g) % LANES
            value = None
            for p in range(4):
                piece = rows[p][:, chunk * LANES : (chunk + 1) * LANES]
                shift = (p * quarter - off) % LANES
                if shift:
                    piece = pltpu.roll(piece, shift, 1)
                value = piece if value is None else jnp.where(lane >= p * quarter, piece, value)
            outs.append(value)
        return outs

    spread(r_in, HALO, HALO + half, half)

    def own_share(b, carry):
        outs = [
            slices([r_in[4 * b + j, :, p * phase : (p + 1) * phase] for p in range(4)])
            for j in range(4)
        ]
        for j in range(4):
            for g in range(groups):
                rshare[g, 4 * b + j] = outs[j][g]
        return carry

    lax.fori_loop(0, half // 4, own_share, 0)
    res_out[...] = rshare[me]

    def detail_block(it, block, own):
        base = 4 * block
        for_sum = None
        weighted = []
        for p in range(4):
            cols = slice(p * phase, (p + 1) * phase)
            ws = [
                xe[base + j, :, cols].astype(jnp.float32) * re[base + j, :, cols] for j in range(4)
            ]
            weighted.append(ws)
            s = (ws[0] + ws[1]) + (ws[2] + ws[3])
            for_sum = s if for_sum is None else for_sum + s
        mean = for_sum * 0.0625
        if own:
            coarse[it, tile, block - HALO // 4] = mean
        for p in range(4):
            for j in range(4):
                det[base + j, :, p * phase : (p + 1) * phase] = weighted[p][j] - mean

    def lat_block(src, dst, block, factor):
        base = 4 * block
        for p in range(4):
            cols = slice(p * phase, (p + 1) * phase)
            rows = [src[base + j, :, cols] for j in range(12)]
            for j in range(4):
                v = kern[0][0] * rows[j + 4]
                for o in range(1, 5):
                    v = v + kern[0][o] * (rows[j + 4 + o] + rows[j + 4 - o])
                if factor is not None:
                    v = v * factor
                dst[base + j, :, cols] = v

    def lon_pass(v):
        plus = [pltpu.roll(a, phase - 1, 1) for a in v]
        minus = [pltpu.roll(a, 1, 1) for a in v]
        table = {0: v, 1: plus, -1: minus}

        def at(t):
            return table[t // 4][t % 4]

        outs = []
        for p in range(4):
            u = kern[1][0] * v[p]
            for o in range(1, 5):
                u = u + kern[1][o] * (at(p + o) + at(p - o))
            outs.append(u)
        return outs

    lon_rows = 4

    def lon_block(src, dst, b):
        rows = [
            [src[b * lon_rows + j, :, p * phase : (p + 1) * phase] for p in range(4)]
            for j in range(lon_rows)
        ]
        outs = [lon_pass(v) for v in rows]
        for j in range(lon_rows):
            for p in range(4):
                dst[b * lon_rows + j, :, p * phase : (p + 1) * phase] = outs[j][p]

    for it in range(ITERS):
        def own_block(b, carry):
            detail_block(it, b, True)
            return carry

        lax.fori_loop(HALO // 4, HALO // 4 + crows, own_block, 0)

        def coarse_send(k, carry):
            other = lax.rem(tile + k, tiles)
            copy(
                coarse.at[it, tile],
                coarse.at[it, tile],
                sem_c.at[it],
                (0, other),
                (1, tile),
                (me, other),
            ).start()
            return carry

        lax.fori_loop(1, tiles, coarse_send, 0)

        if it == 0:

            @pl.when(not_first)
            def _():
                x_down.wait_recv()
                r_down.wait_recv()

            @pl.when(not_last)
            def _():
                x_up.wait_recv()
                r_up.wait_recv()

            spread(rhalo.at[0], 0, hq, hq)
            spread(rhalo.at[1], HALO + height, HALO + height + hq, hq)
        for b in range(HALO // 4):
            detail_block(it, b, False)
            detail_block(it, HALO // 4 + crows + b, False)

        last_block = crows + 1

        def lat_first(b, carry):
            outside = jnp.logical_or(
                jnp.logical_and(b == 0, tile == 0),
                jnp.logical_and(b == last_block, tile == tiles - 1),
            )
            lat_block(det, mid, b, jnp.where(outside, 0.0, 1.0).astype(jnp.float32))
            return carry

        lax.fori_loop(0, crows + 2, lat_first, 0)

        def lat_second(b, carry):
            lat_block(mid, fine, b, None)
            return carry

        lax.fori_loop(0, crows, lat_second, 0)

        def lon_first(b, carry):
            lon_block(fine, mid, b)
            return carry

        def lon_second(b, carry):
            lon_block(mid, fine, b)
            return carry

        lax.fori_loop(0, height // lon_rows, lon_first, 0)
        lax.fori_loop(0, height // lon_rows, lon_second, 0)

        def coarse_wait(k, carry):
            other = lax.rem(tile + k, tiles)
            copy(
                coarse.at[it, other],
                coarse.at[it, other],
                sem_c.at[it],
                (0, other),
                (1, other),
                (me, other),
            ).wait()
            return carry

        lax.fori_loop(1, tiles, coarse_wait, 0)

        def across_tile(t, total):
            total = list(total)
            for b in range(crows):
                v = coarse[it, t, b]
                for a in range(crows):
                    total[a] = total[a] + lat_in[tile * crows + a, t * crows + b] * v
            return tuple(total)

        zero_c = jnp.zeros((fields, phase), jnp.float32)
        across = lax.fori_loop(0, tiles, across_tile, (zero_c,) * crows)
        smooth[...] = jnp.dot(
            jnp.concatenate(across, axis=0),
            lon_in[...],
            precision=exact_mode,
            preferred_element_type=jnp.float32,
        ).reshape(crows, fields, phase)

        def member_sum(block, dot):
            base = 4 * block
            mean = None
            for p in range(4):
                fs = [fine[base + j, :, p * phase : (p + 1) * phase] for j in range(4)]
                s = (fs[0] + fs[1]) + (fs[2] + fs[3])
                mean = s if mean is None else mean + s
            extra = smooth[block] - mean * 0.0625
            rows = []
            for j in range(4):
                row = []
                for p in range(4):
                    cols = slice(p * phase, (p + 1) * phase)
                    u = xe[HALO + base + j, :, cols].astype(jnp.float32) * (
                        fine[base + j, :, cols] + extra
                    )
                    dot = dot + u * re[HALO + base + j, :, cols]
                    row.append(u + swap(u))
                rows.append(row)
            return rows, dot

        def combine(b, dot):
            first, dot = member_sum(b, dot)
            second, dot = member_sum(b + crows // 2, dot)
            for j in range(4):
                packed = [jnp.where(low_p, first[j][p], second[j][p]) for p in range(4)]
                outs = slices(packed)
                for g in range(groups):
                    part[it, g, 4 * b + j] = outs[g]
            return dot

        dot = lax.fori_loop(0, crows // 2, combine, zero_c)
        inner = dot[:, :LANES]
        for c in range(1, phase // LANES):
            inner = inner + dot[:, c * LANES : (c + 1) * LANES]
        residual = res_out[...]
        squares = jnp.sum(residual * residual, axis=0)
        scal[it, flat] = jnp.where(low, squares + swap(squares), inner + swap(inner))

        def scal_copy(other, source):
            return copy(
                scal.at[it, flat],
                scal.at[it, source],
                sem_s.at[it],
                (0, other),
                (1, source),
                (other // tiles, lax.rem(other, tiles)),
            )

        def scal_send(k, carry):
            scal_copy(lax.rem(flat + k, devices), flat).start()
            return carry

        lax.fori_loop(1, devices, scal_send, 0)

        def rs_copy(other, source):
            return copy(
                part.at[it, other],
                rs_recv.at[it, source],
                sem_rs.at[it],
                (0, other),
                (1, source),
                (other, tile),
            )

        def rs_send(k, carry):
            rs_copy(lax.rem(me + k, groups), me).start()
            return carry

        lax.fori_loop(1, groups, rs_send, 0)
        total = part[it, me]

        def rs_wait(k, total):
            other = lax.rem(me + k, groups)
            rs_copy(other, other).wait()
            return total + rs_recv[it, other]

        total = lax.fori_loop(1, groups, rs_wait, total)
        applied = residual + total / (members - 1)
        last = it + 1 == ITERS
        asend[pl.ds(0, half)] = applied
        if not last:
            arecv[me, pl.ds(0, half)] = applied
            for k in range(hq):
                asend[half + k] = jnp.where(
                    low, swap(asend[half - HALO + k]), asend[half - hq + k]
                )
                asend[half + hq + k] = jnp.where(low, asend[k], swap(asend[hq + k]))

            def ag_copy(other, source):
                return copy(
                    asend.at[pl.ds(0, half)],
                    arecv.at[source, pl.ds(0, half)],
                    sem_ag,
                    (0, other),
                    (1, source),
                    (other, tile),
                )

            def down_copy(other, source):
                return copy(
                    asend.at[pl.ds(half, hq)],
                    arecv.at[source, pl.ds(half, hq)],
                    sem_h.at[0],
                    (0, other),
                    (1, source),
                    (other, tile + 1),
                )

            def up_copy(other, source):
                return copy(
                    asend.at[pl.ds(half + hq, hq)],
                    arecv.at[source, pl.ds(half + hq, hq)],
                    sem_h.at[1],
                    (0, other),
                    (1, source),
                    (other, tile - 1),
                )

            def over_groups(condition, start, action):
                @pl.when(condition)
                def _():
                    def step(k, carry):
                        action(lax.rem(me + k, groups))
                        return carry

                    lax.fori_loop(start, groups, step, 0)

            always = tile >= 0
            over_groups(not_last, 0, lambda g: down_copy(g, me).start())
            over_groups(not_first, 0, lambda g: up_copy(g, me).start())
            over_groups(always, 1, lambda g: ag_copy(g, me).start())

        def scal_wait(k, carry):
            other = lax.rem(flat + k, devices)
            scal_copy(other, other).wait()
            return carry

        lax.fori_loop(1, devices, scal_wait, 0)
        sums = lax.fori_loop(
            0, devices, lambda d, t: t + scal[it, d], jnp.zeros((fields, LANES), jnp.float32)
        )
        zero = jnp.zeros_like(sums)
        squares = jnp.sum(jnp.where(low, sums, zero), axis=(0, 1), keepdims=True)
        inner = jnp.sum(jnp.where(low, zero, sums), axis=(0, 1), keepdims=True)
        inner = squares + inner / (members - 1)
        step_size = jnp.broadcast_to(squares / inner, (fields, LANES))
        moved = step_size[None] * residual
        sol_out[...] = moved if it == 0 else sol_out[...] + moved
        res_out[...] = residual - step_size[None] * asend[pl.ds(0, half)]

        if not last:
            over_groups(not_first, 0, lambda g: down_copy(g, g).wait_recv())
            over_groups(not_last, 0, lambda g: up_copy(g, g).wait_recv())
            over_groups(always, 1, lambda g: ag_copy(g, g).wait_recv())
            per = LANES // quarter

            def update(k_base, count, base_low, base_high):
                def rows(b, carry):
                    moves = []
                    for j in range(4):
                        for c in range(phase // LANES):
                            got = [arecv[c * per + i, k_base + 4 * b + j] for i in range(per)]
                            for p in range(4):
                                value = None
                                for i in range(per):
                                    shift = ((i - p) * quarter) % LANES
                                    piece = pltpu.roll(got[i], shift, 1) if shift else got[i]
                                    value = (
                                        piece
                                        if value is None
                                        else jnp.where(lane >= i * quarter, piece, value)
                                    )
                                moves.append((j, p * phase + c * LANES, step_size * value))
                    swapped = [swap(value) for _, _, value in moves]
                    for (j, at, value), other in zip(moves, swapped):
                        cols = slice(at, at + LANES)
                        up, down = base_low + 4 * b + j, base_high + 4 * b + j
                        re[up, :, cols] = re[up, :, cols] - jnp.where(low, value, other)
                        re[down, :, cols] = re[down, :, cols] - jnp.where(low, other, value)
                    return carry

                lax.fori_loop(0, count // 4, rows, 0)

            update(0, half, HALO, HALO + half)
            update(half, hq, 0, hq)
            update(half + hq, hq, HALO + height, HALO + height + hq)
            over_groups(not_last, 0, lambda g: down_copy(g, g).wait_send())
            over_groups(not_first, 0, lambda g: up_copy(g, g).wait_send())
            over_groups(always, 1, lambda g: ag_copy(g, g).wait_send())

    @pl.when(not_last)
    def _():
        x_down.wait_send()
        r_down.wait_send()

    @pl.when(not_first)
    def _():
        x_up.wait_send()
        r_up.wait_send()


def local(perturbations, right_side, fine_taps, coarse_lat, coarse_lon):
    count_local, levels, height, extent = perturbations.shape
    groups, tiles = lax.axis_size("mem"), lax.axis_size("tile")
    members = count_local * groups
    fields = count_local * levels
    half, phase, share = height // 2, extent // 4, extent // groups
    hq, crows, devices = HALO // 2, height // 4, groups * tiles
    assert fields == 8 and share <= LANES and LANES % (share // 4) == 0 and half >= HALO

    natural = jnp.arange(extent)
    order = (natural % 4) * phase + natural // 4
    gather = order[:, None] == natural[None, :]
    x = jnp.einsum(
        "blin,nm->iblm",
        perturbations,
        gather.astype(jnp.bfloat16),
        preferred_element_type=jnp.bfloat16,
    ).reshape(height, fields, extent)
    r = jnp.einsum(
        "lhin,nm->ihlm",
        right_side.reshape(levels, 2, half, extent),
        gather.astype(jnp.float32),
        precision=exact_mode,
    ).reshape(half, fields, extent)

    f32 = jnp.float32
    vmem = pl.BlockSpec(memory_space=pltpu.VMEM)
    smem = pl.BlockSpec(memory_space=pltpu.SMEM)
    sizes = (groups, tiles, levels, height, extent, members)
    dma = pltpu.SemaphoreType.DMA
    sol, res = pl.pallas_call(
        functools.partial(kernel_body, sizes),
        out_shape=[jax.ShapeDtypeStruct((half, fields, LANES), f32)] * 2,
        in_specs=[vmem, vmem, smem, smem, vmem],
        out_specs=[vmem, vmem],
        scratch_shapes=[
            pltpu.VMEM((height + 2 * HALO, fields, extent), jnp.bfloat16),
            pltpu.VMEM((height + 2 * HALO, fields, extent), f32),
            pltpu.VMEM((2, hq, fields, extent), f32),
            pltpu.VMEM((2, hq, fields, extent), f32),
            pltpu.VMEM((height + 2 * HALO, fields, extent), f32),
            pltpu.VMEM((height + HALO, fields, extent), f32),
            pltpu.VMEM((height, fields, extent), f32),
            pltpu.VMEM((ITERS, tiles, crows, fields, phase), f32),
            pltpu.VMEM((crows, fields, phase), f32),
            pltpu.VMEM((ITERS, groups, half, fields, LANES), f32),
            pltpu.VMEM((ITERS, groups, half, fields, LANES), f32),
            pltpu.VMEM((groups, half, fields, LANES), f32),
            pltpu.VMEM((half + 2 * hq, fields, LANES), f32),
            pltpu.VMEM((groups, half + 2 * hq, fields, LANES), f32),
            pltpu.VMEM((ITERS, devices, fields, LANES), f32),
            dma((4,)),
            dma((4,)),
            dma((ITERS, 2, tiles)),
            dma((ITERS, 2, groups)),
            dma((2, groups)),
            dma((2, 2, groups)),
            dma((ITERS, 2, devices)),
        ],
        compiler_params=pltpu.CompilerParams(
            collective_id=0, has_side_effects=True, vmem_limit_bytes=60000 * 1024
        ),
        name="descent",
    )(x, r, fine_taps, coarse_lat, coarse_lon)

    spot = jnp.arange(share)
    place = (spot[:, None] % (share // 4)) * 4 + spot[:, None] // (share // 4) == spot[None, :]

    def natural_order(v):
        v = v[:, :, :share].reshape(half, 2, levels, share)
        return jnp.einsum(
            "ihlm,mn->lhin", v, place.astype(jnp.float32), precision=exact_mode
        ).reshape(levels, height, share)

    return natural_order(sol), natural_order(res)


def solution(mesh):
    placed = (P("mem", None, "tile", None), P(None, "tile", None), P(), P(), P())
    return jax.shard_map(
        local,
        mesh=mesh,
        in_specs=placed,
        out_specs=(P(None, "tile", "mem"), P(None, "tile", "mem")),
        check_vma=False,
    )
```

```python
import functools

import jax
import jax.numpy as jnp
from jax import lax
from jax.experimental import pallas as pl
from jax.experimental.pallas import tpu as pltpu
from jax.sharding import PartitionSpec as P

ITERS = 2
HALO = 8
LANES = 128
MESH = pl.DeviceIdType.MESH

exact_mode = lax.Precision.HIGHEST


def kernel_body(
    sizes,
    x_in,
    r_in,
    taps_in,
    lat_in,
    lon_in,
    sol_out,
    res_out,
    xe,
    re,
    rmsg,
    rhalo,
    det,
    mid,
    fine,
    half_way,
    coarse,
    smooth,
    part,
    rs_recv,
    rshare,
    asend,
    arecv,
    scal,
    sem_x,
    sem_r,
    sem_c,
    sem_rs,
    sem_ag,
    sem_h,
    sem_s,
):
    groups, tiles, levels, height, extent, members = sizes
    me = lax.axis_index("mem")
    tile = lax.axis_index("tile")
    fields = 8
    half = height // 2
    phase = extent // 4
    quarter = extent // groups // 4
    crows = height // 4
    hq = HALO // 2
    devices = groups * tiles
    flat = me * tiles + tile
    not_first = tile > 0
    not_last = tile < tiles - 1

    sub = lax.broadcasted_iota(jnp.int32, (fields, LANES), 0)
    lane = lax.broadcasted_iota(jnp.int32, (fields, LANES), 1)
    low = sub < levels
    low_p = lax.broadcasted_iota(jnp.int32, (fields, phase), 0) < levels
    level_of = lax.rem(lax.broadcasted_iota(jnp.int32, (fields, phase), 0), levels)

    def copy(src, dst, sems, slot_send, slot_recv, target):
        return pltpu.make_async_remote_copy(
            src_ref=src,
            dst_ref=dst,
            send_sem=sems.at[slot_send],
            recv_sem=sems.at[slot_recv],
            device_id=target,
            device_id_type=MESH,
        )

    def swap(v):
        return pltpu.roll(v, levels, 0)

    barrier = pltpu.get_barrier_semaphore()

    def greet(k, carry):
        other = lax.rem(flat + k, devices)
        pl.semaphore_signal(
            barrier,
            inc=1,
            device_id=(other // tiles, lax.rem(other, tiles)),
            device_id_type=MESH,
        )
        return carry

    lax.fori_loop(1, devices, greet, 0)

    kern = []
    for d in range(2):
        raw = []
        for o in range(5):
            v = jnp.full((fields, phase), taps_in[d, 0, o], jnp.float32)
            for l in range(1, levels):
                v = jnp.where(level_of == l, taps_in[d, l, o], v)
            raw.append(v)
        energy = raw[0] * raw[0] + 2.0 * (
            raw[1] * raw[1] + raw[2] * raw[2] + raw[3] * raw[3] + raw[4] * raw[4]
        )
        root = jnp.sqrt(energy)
        kern.append([v / root for v in raw])

    def pack_rows(k, carry):
        a = r_in[half - HALO + k]
        b = r_in[half - hq + k]
        lowx = lax.broadcasted_iota(jnp.int32, (fields, extent), 0) < levels
        rmsg[0, k] = jnp.where(lowx, swap(a), b)
        rmsg[1, k] = jnp.where(lowx, r_in[k], swap(r_in[hq + k]))
        return carry

    lax.fori_loop(0, hq, pack_rows, 0)
    xe[pl.ds(HALO, height)] = x_in[...]

    zero_x = jnp.zeros((HALO, fields, extent), xe.dtype)
    zero_r = jnp.zeros((hq, fields, extent), jnp.float32)

    @pl.when(jnp.logical_not(not_first))
    def _():
        xe[pl.ds(0, HALO)] = zero_x
        rhalo[0] = zero_r
        for g in range(groups):
            arecv[g, pl.ds(half, hq)] = jnp.zeros((hq, fields, LANES), jnp.float32)

    @pl.when(jnp.logical_not(not_last))
    def _():
        xe[pl.ds(HALO + height, HALO)] = zero_x
        rhalo[1] = zero_r
        for g in range(groups):
            arecv[g, pl.ds(half + hq, hq)] = jnp.zeros((hq, fields, LANES), jnp.float32)

    pl.semaphore_wait(barrier, devices - 1)

    x_down = copy(
        x_in.at[pl.ds(height - HALO, HALO)], xe.at[pl.ds(0, HALO)], sem_x, 0, 1, (me, tile + 1)
    )
    x_up = copy(
        x_in.at[pl.ds(0, HALO)], xe.at[pl.ds(HALO + height, HALO)], sem_x, 2, 3, (me, tile - 1)
    )
    r_down = copy(rmsg.at[0], rhalo.at[0], sem_r, 0, 1, (me, tile + 1))
    r_up = copy(rmsg.at[1], rhalo.at[1], sem_r, 2, 3, (me, tile - 1))

    @pl.when(not_last)
    def _():
        x_down.start()
        r_down.start()

    @pl.when(not_first)
    def _():
        x_up.start()
        r_up.start()

    def spread(source, base_low, base_high, count):
        def row(k, carry):
            v = source[k]
            w = swap(v)
            lowx = lax.broadcasted_iota(jnp.int32, (fields, extent), 0) < levels
            re[base_low + k] = jnp.where(lowx, v, w)
            re[base_high + k] = jnp.where(lowx, w, v)
            return carry

        lax.fori_loop(0, count, row, 0)

    def slices(rows):
        outs = []
        for g in range(groups):
            chunk, off = (quarter * g) // LANES, (quarter * g) % LANES
            value = None
            for p in range(4):
                piece = rows[p][:, chunk * LANES : (chunk + 1) * LANES]
                shift = (p * quarter - off) % LANES
                if shift:
                    piece = pltpu.roll(piece, shift, 1)
                value = piece if value is None else jnp.where(lane >= p * quarter, piece, value)
            outs.append(value)
        return outs

    spread(r_in, HALO, HALO + half, half)

    def own_share(b, carry):
        outs = [
            slices([r_in[4 * b + j, :, p * phase : (p + 1) * phase] for p in range(4)])
            for j in range(4)
        ]
        for j in range(4):
            for g in range(groups):
                rshare[g, 4 * b + j] = outs[j][g]
        return carry

    lax.fori_loop(0, half // 4, own_share, 0)
    res_out[...] = rshare[me]

    def detail_block(it, block, own):
        base = 4 * block
        for_sum = None
        weighted = []
        for p in range(4):
            cols = slice(p * phase, (p + 1) * phase)
            ws = [
                xe[base + j, :, cols].astype(jnp.float32) * re[base + j, :, cols] for j in range(4)
            ]
            weighted.append(ws)
            s = (ws[0] + ws[1]) + (ws[2] + ws[3])
            for_sum = s if for_sum is None else for_sum + s
        mean = for_sum * 0.0625
        if own:
            coarse[it, tile, block - HALO // 4] = mean
        for p in range(4):
            for j in range(4):
                det[base + j, :, p * phase : (p + 1) * phase] = weighted[p][j] - mean

    def lat_block(src, dst, block, factor):
        base = 4 * block
        for p in range(4):
            cols = slice(p * phase, (p + 1) * phase)
            rows = [src[base + j, :, cols] for j in range(12)]
            for j in range(4):
                v = kern[0][0] * rows[j + 4]
                for o in range(1, 5):
                    v = v + kern[0][o] * (rows[j + 4 + o] + rows[j + 4 - o])
                if factor is not None:
                    v = v * factor
                dst[base + j, :, cols] = v

    def lon_pass(v):
        plus = [pltpu.roll(a, phase - 1, 1) for a in v]
        minus = [pltpu.roll(a, 1, 1) for a in v]
        table = {0: v, 1: plus, -1: minus}

        def at(t):
            return table[t // 4][t % 4]

        outs = []
        for p in range(4):
            u = kern[1][0] * v[p]
            for o in range(1, 5):
                u = u + kern[1][o] * (at(p + o) + at(p - o))
            outs.append(u)
        return outs

    lon_rows = 4

    def lon_block(src, dst, b):
        rows = [
            [src[b * lon_rows + j, :, p * phase : (p + 1) * phase] for p in range(4)]
            for j in range(lon_rows)
        ]
        outs = [lon_pass(v) for v in rows]
        for j in range(lon_rows):
            for p in range(4):
                dst[b * lon_rows + j, :, p * phase : (p + 1) * phase] = outs[j][p]

    for it in range(ITERS):
        def own_block(b, carry):
            detail_block(it, b, True)
            return carry

        lax.fori_loop(HALO // 4, HALO // 4 + crows, own_block, 0)

        def coarse_send(k, carry):
            other = lax.rem(tile + k, tiles)
            copy(
                coarse.at[it, tile],
                coarse.at[it, tile],
                sem_c.at[it],
                (0, other),
                (1, tile),
                (me, other),
            ).start()
            return carry

        lax.fori_loop(1, tiles, coarse_send, 0)

        last_block = crows + 1

        def lat_first(b, carry):
            outside = jnp.logical_or(
                jnp.logical_and(b == 0, tile == 0),
                jnp.logical_and(b == last_block, tile == tiles - 1),
            )
            lat_block(det, mid, b, jnp.where(outside, 0.0, 1.0).astype(jnp.float32))
            return carry

        def lat_second(b, carry):
            lat_block(mid, fine, b, None)
            return carry

        def lon_first(b, carry):
            lon_block(fine, half_way, b)
            return carry

        def lon_second(b, carry):
            lon_block(half_way, fine, b)
            return carry

        edge = HALO // 4
        lax.fori_loop(edge, crows, lat_first, 0)
        for body in (lat_second, lon_first, lon_second):
            lax.fori_loop(edge, crows - edge, body, 0)

        if it == 0:

            @pl.when(not_first)
            def _():
                x_down.wait_recv()
                r_down.wait_recv()

            @pl.when(not_last)
            def _():
                x_up.wait_recv()
                r_up.wait_recv()

            spread(rhalo.at[0], 0, hq, hq)
            spread(rhalo.at[1], HALO + height, HALO + height + hq, hq)
        else:
            over_groups(not_first, 0, lambda g: down_copy(g, g).wait_recv())
            over_groups(not_last, 0, lambda g: up_copy(g, g).wait_recv())
            update(half, hq, 0, hq)
            update(half + hq, hq, HALO + height, HALO + height + hq)
        for b in range(HALO // 4):
            detail_block(it, b, False)
            detail_block(it, HALO // 4 + crows + b, False)


        lax.fori_loop(0, edge, lat_first, 0)
        lax.fori_loop(crows, crows + edge, lat_first, 0)
        for body in (lat_second, lon_first, lon_second):
            lax.fori_loop(0, edge, body, 0)
            lax.fori_loop(crows - edge, crows, body, 0)

        def coarse_wait(k, carry):
            other = lax.rem(tile + k, tiles)
            copy(
                coarse.at[it, other],
                coarse.at[it, other],
                sem_c.at[it],
                (0, other),
                (1, other),
                (me, other),
            ).wait()
            return carry

        lax.fori_loop(1, tiles, coarse_wait, 0)

        def across_tile(t, total):
            total = list(total)
            for b in range(crows):
                v = coarse[it, t, b]
                for a in range(crows):
                    total[a] = total[a] + lat_in[tile * crows + a, t * crows + b] * v
            return tuple(total)

        zero_c = jnp.zeros((fields, phase), jnp.float32)
        across = lax.fori_loop(0, tiles, across_tile, (zero_c,) * crows)
        smooth[...] = jnp.dot(
            jnp.concatenate(across, axis=0),
            lon_in[...],
            precision=exact_mode,
            preferred_element_type=jnp.float32,
        ).reshape(crows, fields, phase)

        def member_sum(block, dot):
            base = 4 * block
            mean = None
            for p in range(4):
                fs = [fine[base + j, :, p * phase : (p + 1) * phase] for j in range(4)]
                s = (fs[0] + fs[1]) + (fs[2] + fs[3])
                mean = s if mean is None else mean + s
            extra = smooth[block] - mean * 0.0625
            rows = []
            for j in range(4):
                row = []
                for p in range(4):
                    cols = slice(p * phase, (p + 1) * phase)
                    u = xe[HALO + base + j, :, cols].astype(jnp.float32) * (
                        fine[base + j, :, cols] + extra
                    )
                    dot = dot + u * re[HALO + base + j, :, cols]
                    row.append(u + swap(u))
                rows.append(row)
            return rows, dot

        def rs_copy(chunk, other, source):
            rows = pl.ds(4 * chunk, 4)
            return copy(
                part.at[it, other, rows],
                rs_recv.at[it, source, rows],
                sem_rs.at[it],
                (0, chunk, other),
                (1, chunk, source),
                (other, tile),
            )

        def combine(b, dot):
            first, dot = member_sum(b, dot)
            second, dot = member_sum(b + crows // 2, dot)
            for j in range(4):
                packed = [jnp.where(low_p, first[j][p], second[j][p]) for p in range(4)]
                outs = slices(packed)
                for g in range(groups):
                    part[it, g, 4 * b + j] = outs[g]

            def rs_send(k, carry):
                rs_copy(b, lax.rem(me + k, groups), me).start()
                return carry

            lax.fori_loop(1, groups, rs_send, 0)
            return dot

        dot = lax.fori_loop(0, crows // 2, combine, zero_c)
        inner = dot[:, :LANES]
        for c in range(1, phase // LANES):
            inner = inner + dot[:, c * LANES : (c + 1) * LANES]
        residual = res_out[...]
        squares = jnp.sum(residual * residual, axis=0)
        scal[it, flat] = jnp.where(low, squares + swap(squares), inner + swap(inner))

        def scal_copy(other, source):
            return copy(
                scal.at[it, flat],
                scal.at[it, source],
                sem_s.at[it],
                (0, other),
                (1, source),
                (other // tiles, lax.rem(other, tiles)),
            )

        def scal_send(k, carry):
            scal_copy(lax.rem(flat + k, devices), flat).start()
            return carry

        lax.fori_loop(1, devices, scal_send, 0)

        total = part[it, me]

        def rs_wait(k, total):
            other = lax.rem(me + k, groups)
            for chunk in range(crows // 2):
                rs_copy(chunk, other, other).wait()
            return total + rs_recv[it, other]

        total = lax.fori_loop(1, groups, rs_wait, total)
        applied = residual + total / (members - 1)
        last = it + 1 == ITERS
        asend[pl.ds(0, half)] = applied
        if not last:
            arecv[me, pl.ds(0, half)] = applied
            for k in range(hq):
                asend[half + k] = jnp.where(
                    low, swap(asend[half - HALO + k]), asend[half - hq + k]
                )
                asend[half + hq + k] = jnp.where(low, asend[k], swap(asend[hq + k]))

            def ag_copy(other, source):
                return copy(
                    asend.at[pl.ds(0, half)],
                    arecv.at[source, pl.ds(0, half)],
                    sem_ag,
                    (0, other),
                    (1, source),
                    (other, tile),
                )

            def down_copy(other, source):
                return copy(
                    asend.at[pl.ds(half, hq)],
                    arecv.at[source, pl.ds(half, hq)],
                    sem_h.at[0],
                    (0, other),
                    (1, source),
                    (other, tile + 1),
                )

            def up_copy(other, source):
                return copy(
                    asend.at[pl.ds(half + hq, hq)],
                    arecv.at[source, pl.ds(half + hq, hq)],
                    sem_h.at[1],
                    (0, other),
                    (1, source),
                    (other, tile - 1),
                )

            def over_groups(condition, start, action):
                @pl.when(condition)
                def _():
                    def step(k, carry):
                        action(lax.rem(me + k, groups))
                        return carry

                    lax.fori_loop(start, groups, step, 0)

            always = tile >= 0
            over_groups(always, 1, lambda g: ag_copy(g, me).start())
            over_groups(not_last, 0, lambda g: down_copy(g, me).start())
            over_groups(not_first, 0, lambda g: up_copy(g, me).start())

        def scal_wait(k, carry):
            other = lax.rem(flat + k, devices)
            scal_copy(other, other).wait()
            return carry

        lax.fori_loop(1, devices, scal_wait, 0)
        sums = lax.fori_loop(
            0, devices, lambda d, t: t + scal[it, d], jnp.zeros((fields, LANES), jnp.float32)
        )
        zero = jnp.zeros_like(sums)
        squares = jnp.sum(jnp.where(low, sums, zero), axis=(0, 1), keepdims=True)
        inner = jnp.sum(jnp.where(low, zero, sums), axis=(0, 1), keepdims=True)
        inner = squares + inner / (members - 1)
        step_size = jnp.broadcast_to(squares / inner, (fields, LANES))
        moved = step_size[None] * residual
        sol_out[...] = moved if it == 0 else sol_out[...] + moved
        res_out[...] = residual - step_size[None] * asend[pl.ds(0, half)]

        if not last:
            over_groups(always, 1, lambda g: ag_copy(g, g).wait_recv())
            per = LANES // quarter

            def update(k_base, count, base_low, base_high):
                def rows(b, carry):
                    moves = []
                    for j in range(4):
                        for c in range(phase // LANES):
                            got = [arecv[c * per + i, k_base + 4 * b + j] for i in range(per)]
                            for p in range(4):
                                value = None
                                for i in range(per):
                                    shift = ((i - p) * quarter) % LANES
                                    piece = pltpu.roll(got[i], shift, 1) if shift else got[i]
                                    value = (
                                        piece
                                        if value is None
                                        else jnp.where(lane >= i * quarter, piece, value)
                                    )
                                moves.append((j, p * phase + c * LANES, step_size * value))
                    swapped = [swap(value) for _, _, value in moves]
                    for (j, at, value), other in zip(moves, swapped):
                        cols = slice(at, at + LANES)
                        up, down = base_low + 4 * b + j, base_high + 4 * b + j
                        re[up, :, cols] = re[up, :, cols] - jnp.where(low, value, other)
                        re[down, :, cols] = re[down, :, cols] - jnp.where(low, other, value)
                    return carry

                lax.fori_loop(0, count // 4, rows, 0)

            update(0, half, HALO, HALO + half)
            over_groups(not_last, 0, lambda g: down_copy(g, g).wait_send())
            over_groups(not_first, 0, lambda g: up_copy(g, g).wait_send())
            over_groups(always, 1, lambda g: ag_copy(g, g).wait_send())

    @pl.when(not_last)
    def _():
        x_down.wait_send()
        r_down.wait_send()

    @pl.when(not_first)
    def _():
        x_up.wait_send()
        r_up.wait_send()


def local(perturbations, right_side, fine_taps, coarse_lat, coarse_lon):
    count_local, levels, height, extent = perturbations.shape
    groups, tiles = lax.axis_size("mem"), lax.axis_size("tile")
    members = count_local * groups
    fields = count_local * levels
    half, phase, share = height // 2, extent // 4, extent // groups
    hq, crows, devices = HALO // 2, height // 4, groups * tiles
    assert fields == 8 and share <= LANES and LANES % (share // 4) == 0 and half >= HALO

    natural = jnp.arange(extent)
    order = (natural % 4) * phase + natural // 4
    gather = order[:, None] == natural[None, :]
    x = jnp.einsum(
        "blin,nm->iblm",
        perturbations,
        gather.astype(jnp.bfloat16),
        preferred_element_type=jnp.bfloat16,
    ).reshape(height, fields, extent)
    r = jnp.einsum(
        "lhin,nm->ihlm",
        right_side.reshape(levels, 2, half, extent),
        gather.astype(jnp.float32),
        precision=exact_mode,
    ).reshape(half, fields, extent)

    f32 = jnp.float32
    vmem = pl.BlockSpec(memory_space=pltpu.VMEM)
    smem = pl.BlockSpec(memory_space=pltpu.SMEM)
    sizes = (groups, tiles, levels, height, extent, members)
    dma = pltpu.SemaphoreType.DMA
    sol, res = pl.pallas_call(
        functools.partial(kernel_body, sizes),
        out_shape=[jax.ShapeDtypeStruct((half, fields, LANES), f32)] * 2,
        in_specs=[vmem, vmem, smem, smem, vmem],
        out_specs=[vmem, vmem],
        scratch_shapes=[
            pltpu.VMEM((height + 2 * HALO, fields, extent), jnp.bfloat16),
            pltpu.VMEM((height + 2 * HALO, fields, extent), f32),
            pltpu.VMEM((2, hq, fields, extent), f32),
            pltpu.VMEM((2, hq, fields, extent), f32),
            pltpu.VMEM((height + 2 * HALO, fields, extent), f32),
            pltpu.VMEM((height + HALO, fields, extent), f32),
            pltpu.VMEM((height, fields, extent), f32),
            pltpu.VMEM((height, fields, extent), f32),
            pltpu.VMEM((ITERS, tiles, crows, fields, phase), f32),
            pltpu.VMEM((crows, fields, phase), f32),
            pltpu.VMEM((ITERS, groups, half, fields, LANES), f32),
            pltpu.VMEM((ITERS, groups, half, fields, LANES), f32),
            pltpu.VMEM((groups, half, fields, LANES), f32),
            pltpu.VMEM((half + 2 * hq, fields, LANES), f32),
            pltpu.VMEM((groups, half + 2 * hq, fields, LANES), f32),
            pltpu.VMEM((ITERS, devices, fields, LANES), f32),
            dma((4,)),
            dma((4,)),
            dma((ITERS, 2, tiles)),
            dma((ITERS, 2, crows // 2, groups)),
            dma((2, groups)),
            dma((2, 2, groups)),
            dma((ITERS, 2, devices)),
        ],
        compiler_params=pltpu.CompilerParams(
            collective_id=0, has_side_effects=True, vmem_limit_bytes=60000 * 1024
        ),
        name="descent",
    )(x, r, fine_taps, coarse_lat, coarse_lon)

    spot = jnp.arange(share)
    place = (spot[:, None] % (share // 4)) * 4 + spot[:, None] // (share // 4) == spot[None, :]

    def natural_order(v):
        v = v[:, :, :share].reshape(half, 2, levels, share)
        return jnp.einsum(
            "ihlm,mn->lhin", v, place.astype(jnp.float32), precision=exact_mode
        ).reshape(levels, height, share)

    return natural_order(sol), natural_order(res)


def solution(mesh):
    placed = (P("mem", None, "tile", None), P(None, "tile", None), P(), P(), P())
    return jax.shard_map(
        local,
        mesh=mesh,
        in_specs=placed,
        out_specs=(P(None, "tile", "mem"), P(None, "tile", "mem")),
        check_vma=False,
    )
```
